32 devices in a mesh: replica: 2 (over x), expert: 8 (over z, y), sub: 2 (over core).
Axes of the slice: x: 2, y: 2, z: 4, core: 2. Of those that a mesh axis runs over, the one named last changes fastest.
Arguments:
- tokens: bfloat16 [256, 7168], P(('replica', 'expert', 'sub')), parts along dimension 0, may hold values from -6 to 6
- expert_ids: int32 [256, 2], P(('replica', 'expert', 'sub')), parts along dimension 0, may hold values from 0 to 3, all different within a row; in each aligned block of 8 rows (0 to 7, 8 to 15, ...) at most 6 rows name the same one
- route_levels: int32 [256, 2], P(('replica', 'expert', 'sub')), parts along dimension 0, may hold values from 1 to 255
- gate_proj: bfloat16 [8, 7168, 512], P('expert', None, 'sub'), may hold values from -0.0625 to 0.0625
- up_proj: bfloat16 [8, 7168, 512], P('expert', None, 'sub'), may hold values from -0.0625 to 0.0625
- down_proj: bfloat16 [8, 512, 7168], P('expert', 'sub'), may hold values from -0.1875 to 0.1875
Outputs:
- moe_out: bfloat16 [256, 7168], P(('replica', 'expert', 'sub')), parts along dimension 0
The draws below stay inside these ranges and needn't reach their ends.
There are 2 independent parts, one for each index of `replica`. The reference program is written for one: setup_inputs(seed, part) draws one part's arguments, and reference() takes and returns one part's arrays. A program takes and returns all parts, laid end to end along the dimension named above; an argument that names none is the same for every part. Nothing has to cross between parts.
Inputs may be any that keep to these rules, and one draw needn't show every extreme that they name: `expert_ids`: each row names 2 different experts; among the 8 rows of one device no expert is named more than 6 times, and in some devices' rows one is named exactly 6 times.
All inputs are finite; a program needn't handle non-finite values.
Results may differ from the reference program's by a relative error of at most 0.013.
Values may be sent and summed in bfloat16 or wider, within the bound.
A program may use at most 448 MiB of HBM per device.

```python
import math
import jax
import jax.numpy as jnp
import numpy as np
from jax import lax

D = 7168
FF = 1024
TOK_DEV = 8
EXPERTS = 4
TOPK = 2
CAP = 6
TOKENS = 128
N_EXPERT = 8
N_SUB = 2


def set_ends(array, rng, least, top_value):
    shape = array.shape
    spot = [jax.random.randint(jax.random.fold_in(rng, axis), (), 0, shape[axis]) for axis in range(len(shape))]
    array = array.at[tuple(spot)].set(least)
    longest = shape.index(max(shape))
    spot[longest] = (spot[longest] + 1) % shape[longest]
    return array.at[tuple(spot)].set(top_value)


def block_levels(own_key, shape, cuts, smallest, largest):
    level, own = 1.0, jax.random.fold_in(own_key, 6)
    for dim, parts in cuts:
        draws = jnp.exp(jax.random.uniform(jax.random.fold_in(own, dim), (parts,), jnp.float32, smallest / len(cuts), largest / len(cuts)))
        level = level * jnp.repeat(draws, shape[dim] // parts).reshape([-1 if axis == dim else 1 for axis in range(len(shape))])
    return level


def deal_out(key, own, number, rows, amount, top, bound, lean):
    ranking = jax.random.permutation(key, amount)
    heavy_load, common = portions_of(amount, rows * top, bound, lean, True), portions_of(amount, rows * top, bound, lean, False)
    places = jnp.arange(amount)

    def named(lengths, offset_by):
        used = int((lengths > 0).sum())
        fixed = max(1, used // 4)
        passed = fixed + (places - fixed + offset_by * (used - fixed)) % max(1, amount - fixed)
        return jnp.zeros((amount,), jnp.int32).at[ranking[jnp.where(places < fixed, places, passed)]].set(jnp.asarray(lengths, jnp.int32))

    lengths = jnp.where(number % 4 == 0, named(heavy_load, number // 4), named(common, number - number // 4 - 1))
    mixed = jax.random.permutation(jax.random.fold_in(own, 3), amount)
    giver, taker = mixed[0:amount // 2 * 2:2], mixed[1:amount // 2 * 2:2]
    room = jnp.minimum(lengths[giver] - 1, bound - lengths[taker]) // 2
    room = jnp.where((giver == ranking[0]) | (taker == ranking[0]) | (lengths[taker] == 0), 0, jnp.maximum(room, 0))
    passed = jax.random.randint(jax.random.fold_in(own, 4), (amount // 2,), 0, 1 << 20) % (room + 1)
    lengths = lengths.at[giver].add(-passed).at[taker].add(passed)
    labels = jnp.searchsorted(jnp.cumsum(lengths), jnp.arange(rows * top), side="right").astype(jnp.int32)
    grid = labels.reshape(top, rows).T
    grid = grid[jax.random.permutation(jax.random.fold_in(own, 1), rows)]
    offset_by = jax.random.randint(jax.random.fold_in(own, 2), (rows, 1), 0, top)
    return jnp.take_along_axis(grid, (jnp.arange(top)[None, :] + offset_by) % top, axis=1)


def portions_of(count, total, bound, slope, full):
    portions = [(1 << 20) // math.isqrt(grade ** slope) + 1 for grade in range(1, count + 1)]
    largest = bound if full else min(bound, max(-(-total // count), total * portions[0] // sum(portions)))
    least = 1 if total - largest >= count - 1 else 0
    holding, surplus = [largest] + [least] * (count - 1), total - largest - least * (count - 1)
    while surplus > 0:
        free = [i for i in range(1, count) if holding[i] < largest] or [i for i in range(1, count) if holding[i] < bound]
        mass, budget = sum([portions[i] for i in free]), surplus
        for i in free:
            addition = min(bound - holding[i], max(1, budget * portions[i] // mass), surplus)
            holding[i] = holding[i] + addition
            surplus = surplus - addition
    return np.array(holding)


def noise(rng, dims, scale, most, split=(), held_as=jnp.bfloat16):
    drawn = jax.random.normal(rng, dims, jnp.float32) * scale
    if len(split) > 0:
        drawn = block_levels(rng, dims, split, -0.22, 0.18) * drawn
    return jnp.clip(drawn, min=-most, max=most).astype(held_as)


def setup_inputs(seed: int = 0, part: int = 0) -> dict:
    splits = jax.random.split(jax.random.key(seed), 7)
    own_keys = jax.random.split(jax.random.fold_in(splits[6], part), 7)
    tokens = noise(own_keys[0], (TOKENS, D), 1.0, 6.0, ((0, 16),))
    expert_ids_keys = jax.random.split(jax.random.fold_in(own_keys[1], 1), TOKENS // TOK_DEV)
    expert_ids_turns = jax.random.permutation(jax.random.fold_in(own_keys[1], 3), TOKENS // TOK_DEV)
    expert_ids = jax.vmap(lambda own, number: deal_out(jax.random.fold_in(own_keys[1], 2), own, number, TOK_DEV, EXPERTS, TOPK, CAP, 2))(expert_ids_keys, expert_ids_turns).reshape((TOKENS, TOPK))
    route_levels = set_ends(jax.random.randint(own_keys[2], (TOKENS, TOPK), 1, 256), jax.random.fold_in(own_keys[2], 1), 1, 255).astype(jnp.int32)
    gate_proj = noise(splits[3], (2 * EXPERTS, D, FF // 2), D ** -0.5, 0.0625, ((0, 8), (2, 2)))
    up_proj = noise(splits[4], (2 * EXPERTS, D, FF // 2), D ** -0.5, 0.0625, ((0, 8), (2, 2)))
    down_proj = noise(splits[5], (2 * EXPERTS, FF // 2, D), FF ** -0.5, 0.1875, ((0, 8), (1, 2)))
    return {"tokens": tokens, "expert_ids": expert_ids, "route_levels": route_levels, "gate_proj": gate_proj, "up_proj": up_proj, "down_proj": down_proj}


def reference(tokens, expert_ids, route_levels, gate_proj, up_proj, down_proj):
    devices = N_EXPERT * N_SUB
    quarter = FF // 4
    source = tokens.reshape(devices, TOK_DEV, D).astype(jnp.float32)
    picked = expert_ids.reshape(devices, TOK_DEV * TOPK)
    onehot = (picked[:, :, None] == jnp.arange(EXPERTS, dtype=jnp.int32)[None, None, :]).astype(jnp.int32)
    before = jnp.cumsum(onehot, axis=1, dtype=jnp.int32) - onehot
    slot_of = jnp.sum(before * onehot, axis=2)
    shares = route_levels.astype(jnp.float32)
    shares = shares / jnp.sum(shares, axis=1, keepdims=True)
    shares = shares.reshape(devices, TOK_DEV, TOPK)
    slot_range = jnp.arange(CAP, dtype=jnp.int32)

    def advance(running, expert):
        chosen = (picked == expert)[:, :, None] & (slot_of[:, :, None] == slot_range[None, None, :])
        placed = chosen.astype(jnp.float32).reshape(devices, TOK_DEV, TOPK, CAP)
        sender = jnp.sum(placed, axis=2)
        weighting = jnp.sum(placed * shares[:, :, :, None], axis=2)
        slot_rows = jnp.einsum("dtc,dtf->dcf", sender, source).astype(jnp.bfloat16).reshape(devices * CAP, D)
        index_low = (2 * expert).astype(jnp.int32)
        index_high = (2 * expert + 1).astype(jnp.int32)
        gate_full = jnp.concatenate([lax.dynamic_index_in_dim(gate_proj, index_low, 0, keepdims=False),
                                     lax.dynamic_index_in_dim(gate_proj, index_high, 0, keepdims=False)], axis=1)
        up_full = jnp.concatenate([lax.dynamic_index_in_dim(up_proj, index_low, 0, keepdims=False),
                                   lax.dynamic_index_in_dim(up_proj, index_high, 0, keepdims=False)], axis=1)
        down_full = jnp.concatenate([lax.dynamic_index_in_dim(down_proj, index_low, 0, keepdims=False),
                                     lax.dynamic_index_in_dim(down_proj, index_high, 0, keepdims=False)], axis=0)
        gate_vals = jnp.dot(slot_rows, gate_full, preferred_element_type=jnp.float32)
        up_vals = jnp.dot(slot_rows, up_full, preferred_element_type=jnp.float32)
        hidden = (jax.nn.silu(gate_vals) * up_vals).astype(jnp.bfloat16)
        summed = jnp.zeros((devices * CAP, D), jnp.float32)
        for portion in range(4):
            piece = jnp.dot(hidden[:, portion * quarter:(portion + 1) * quarter],
                            down_full[portion * quarter:(portion + 1) * quarter],
                            preferred_element_type=jnp.float32).astype(jnp.bfloat16)
            piece = lax.optimization_barrier(piece)
            summed = summed + piece.astype(jnp.float32)
        rounded = lax.optimization_barrier(summed.astype(jnp.bfloat16))
        expert_out = rounded.astype(jnp.float32).reshape(devices, CAP, D)
        running = running + jnp.einsum("dtc,dcf->dtf", weighting, expert_out, precision=lax.Precision.HIGHEST)
        return running, None

    start = jnp.zeros((devices, TOK_DEV, D), jnp.float32)
    running, _ = lax.scan(advance, start, jnp.arange(EXPERTS, dtype=jnp.int32))
    return running.reshape(devices * TOK_DEV, D).astype(jnp.bfloat16)
```

```python
import functools
import jax
import jax.numpy as jnp
from jax import lax
from jax.experimental import pallas as pl
from jax.experimental.pallas import tpu as pltpu
from jax.sharding import PartitionSpec as P


def local(tokens, expert_ids, route_levels, gate_proj, up_proj, down_proj):
    rows_here, width = tokens.shape
    picks = expert_ids.shape[1]
    experts = lax.axis_size("expert") * lax.axis_size("sub") // 4
    capacity = rows_here * picks * 3 // (experts * 2)
    pair_count = rows_here * picks
    flat_ids = expert_ids.reshape(pair_count)
    onehot = (flat_ids[:, None] == jnp.arange(experts, dtype=jnp.int32)[None, :]).astype(jnp.int32)
    before = jnp.cumsum(onehot, axis=0, dtype=jnp.int32) - onehot
    slot_of = jnp.sum(before * onehot, axis=1)
    position = flat_ids * capacity + slot_of
    placed = (position[:, None] == jnp.arange(experts * capacity, dtype=jnp.int32)[None, :]).astype(
        jnp.float32
    )
    shares = route_levels.astype(jnp.float32)
    shares = shares / jnp.sum(shares, axis=1, keepdims=True)
    owner_rows = (
        jnp.arange(pair_count, dtype=jnp.int32)[None, :] // picks
        == jnp.arange(rows_here, dtype=jnp.int32)[:, None]
    ).astype(jnp.float32)
    sender = jnp.dot(owner_rows, placed, precision=lax.Precision.HIGHEST)
    weighting = jnp.dot(
        owner_rows * shares.reshape(1, pair_count), placed, precision=lax.Precision.HIGHEST
    )
    outgoing = jnp.dot(sender.T.astype(jnp.bfloat16), tokens, preferred_element_type=jnp.float32)
    outgoing = outgoing.astype(jnp.bfloat16).reshape(experts, 1, capacity, width)
    gate_local = gate_proj[0]
    up_local = up_proj[0]
    down_local = down_proj[0]
    buffer = jnp.broadcast_to(outgoing, (experts, 4, capacity, width)).reshape(
        4 * experts, capacity, width
    )
    arrived = lax.all_to_all(buffer, ("expert", "sub"), split_axis=0, concat_axis=0, tiled=True)
    items = arrived.shape[1]
    leading = arrived.shape[:-1]
    flat_rows = arrived.reshape(-1, width)
    gate_vals = jnp.dot(flat_rows, gate_local, preferred_element_type=jnp.float32)
    up_vals = jnp.dot(flat_rows, up_local, preferred_element_type=jnp.float32)
    hidden = (jax.nn.silu(gate_vals) * up_vals).astype(jnp.bfloat16)
    terms = jnp.dot(hidden, down_local, preferred_element_type=jnp.float32).astype(jnp.bfloat16)
    terms = terms.reshape(leading + (width,)).reshape(-1, 2, items, width)
    groups, _, items, _ = terms.shape
    flat_terms = terms.reshape(2 * groups, items, width)
    returned = lax.all_to_all(
        flat_terms, ("expert", "sub"), split_axis=0, concat_axis=0, tiled=True
    )
    results = jnp.sum(returned.reshape(experts, -1, capacity, width), axis=1, dtype=jnp.float32)
    rounded = lax.optimization_barrier(
        results.reshape(experts * capacity, width).astype(jnp.bfloat16)
    )
    mixed = jnp.dot(
        weighting,
        rounded.astype(jnp.float32),
        precision=lax.Precision.HIGHEST,
        preferred_element_type=jnp.float32,
    )
    return mixed.astype(jnp.bfloat16)


MESH = pl.DeviceIdType.MESH
VMEM_BUDGET = 60 * 1024 * 1024


def column_cuts(width, pieces):
    lanes = width // 128
    edges = [128 * (lanes * i // pieces) for i in range(pieces + 1)]
    return [(a, b - a) for a, b in zip(edges[:-1], edges[1:]) if b > a]


def fused(groups, p_width, cuts, ids_ref, levels_ref, tok_in, gate_hbm, up_hbm, down_hbm, out_ref,
          tok, gate_v, up_v, down_v, hid, keep, dsend, drecv, ysend, yrecv, zsend, zrecv,
          send_sem, recv_sem, local_sem):
    rows, width = tok_in.shape
    spot = lax.axis_index("expert")
    s = lax.axis_index("sub")
    z, h = spot // 2, spot % 2
    n = groups

    loads = [pltpu.make_async_copy(src, dst, local_sem.at[i]) for i, (src, dst) in enumerate(
        ((gate_hbm.at[0], gate_v), (up_hbm.at[0], up_v), (down_hbm.at[0], down_v)))]
    for load in loads:
        load.start()
    tok[spot, s] = tok_in[...]

    def ring(step):
        return lax.rem(z + step + n, n)

    def at(group, half, core):
        return {"expert": group * 2 + half, "sub": core}

    sub_peer, half_peer = at(z, h, 1 - s), at(z, 1 - h, s)
    barrier = pltpu.get_barrier_semaphore()
    peers = [sub_peer, half_peer] + [at(ring(d), h, s) for d in range(1, n)]
    for peer in peers:
        pl.semaphore_signal(barrier, inc=1, device_id=peer, device_id_type=MESH)
    pl.semaphore_wait(barrier, len(peers))

    count = [0]
    started = []

    def send(src, dst, peer):
        i = count[0]
        count[0] += 1
        copy = pltpu.make_async_remote_copy(src_ref=src, dst_ref=dst, send_sem=send_sem.at[i],
                                            recv_sem=recv_sem.at[i], device_id=peer, device_id_type=MESH)
        copy.start()
        started.append(copy)
        return copy

    def block(group, half, cols):
        return tok.at[group * 2 + half, s, :, pl.ds(cols[0], cols[1])]

    def move(group, half, cols, peer):
        return send(block(group, half, cols), block(group, half, cols), peer)

    def own(cols, peer):
        return send(tok_in.at[:, pl.ds(cols[0], cols[1])], block(z, h, cols), peer)

    P, Q = (0, p_width), (p_width, width - p_width)
    last = []

    def across(group, half, cols):
        last.append(move(group, half, cols, sub_peer))

    def halves(cols):
        first = cols[1] // 256 * 128
        return (cols[0], first), (cols[0] + first, cols[1] - first)

    up_peer, down_peer = at(ring(1), h, s), at(ring(-1), h, s)

    def hop(half, cols, first):
        def starter(d):
            a, b = (cols, cols) if 2 * d < n else halves(cols)
            if d == 1 and first:
                return [own(a, up_peer), own(b, down_peer)]
            return [move(ring(1 - d), half, a, up_peer), move(ring(d - 1), half, b, down_peer)]
        return starter

    y_p = own(P, half_peer)
    hop_p, hop_q, hop_o = hop(h, P, True), hop(h, Q, True), hop(1 - h, P, False)
    step_p = hop_p(1)
    step_q = hop_q(1)
    y_q = [own(Q, half_peer)]
    last.append(send(tok_in, tok.at[spot, s], sub_peer))
    y_p.wait_recv()
    step_o = hop_o(1)
    across(z, 1 - h, P)
    for d in range(1, n // 2 + 1):
        for name in ("p", "q", "o"):
            steps = {"p": step_p, "q": step_q, "o": step_o}[name]
            for copy in steps:
                copy.wait_recv()
            cols = Q if name == "q" else P
            half = 1 - h if name == "o" else h
            if 2 * d < n:
                more = {"p": hop_p, "q": hop_q, "o": hop_o}[name](d + 1)
                if name == "p":
                    step_p = more
                elif name == "q":
                    step_q = more
                else:
                    step_o = more
                arrived = [ring(-d), ring(d)]
            else:
                arrived = [ring(d)]
            for group in arrived:
                if name == "q":
                    y_q.append(move(group, half, cols, half_peer))
                across(group, half, cols)
    order = [z]
    for d in range(1, n // 2 + 1):
        order += [ring(-d), ring(d)] if 2 * d < n else [ring(d)]
    for copy, group in zip(y_q, order):
        copy.wait_recv()
        across(group, 1 - h, Q)
    for copy in last:
        copy.wait_recv()
    for load in loads:
        load.wait()

    total = 4 * n * rows
    gate = jnp.zeros((total, gate_v.shape[1]), jnp.float32)
    up = jnp.zeros((total, up_v.shape[1]), jnp.float32)
    for start, size in cuts:
        lhs = tok[:, :, :, start:start + size].reshape(total, size)
        gate += jnp.dot(lhs, gate_v[start:start + size, :], preferred_element_type=jnp.float32)
        up += jnp.dot(lhs, up_v[start:start + size, :], preferred_element_type=jnp.float32)
    hid[...] = (jax.nn.silu(gate) * up).reshape(hid.shape)
    units = hid.shape[-1]
    ordered = jnp.concatenate([hid[:, half, core].reshape(n * rows, units)
                               for core in (1 - s, s) for half in (1 - h, h)], axis=0).astype(jnp.bfloat16)

    part, span = n * rows, max(size for _, size in cuts)
    d_copies, y_copies, z_copies = [], [], []
    for c, (start, size) in enumerate(cuts):
        terms = jnp.dot(ordered, down_v[:, start:start + size], preferred_element_type=jnp.float32)
        dsend[c] = terms[:2 * part].astype(jnp.bfloat16)
        keep[c] = terms[2 * part:]
        d_copies.append(send(dsend.at[c], drecv.at[c], sub_peer))
    for c in range(len(cuts)):
        d_copies[c].wait_recv()
        ysend[c] = (keep[c, :part] + drecv[c, :part].astype(jnp.float32)).astype(jnp.bfloat16)
        y_copies.append(send(ysend.at[c], yrecv.at[c], half_peer))
    for c in range(len(cuts)):
        y_copies[c].wait_recv()
        sums = (keep[c, part:] + drecv[c, part:].astype(jnp.float32)) + yrecv[c].astype(jnp.float32)
        zsend[c] = sums.reshape(n, rows, span).astype(jnp.bfloat16)
        z_copies.append([send(zsend.at[c, ring(d)], zrecv.at[c, d], at(ring(d), h, s)) for d in range(1, n)])
    levels = levels_ref[...].astype(jnp.float32)
    shares = levels / jnp.sum(levels, axis=1, keepdims=True)
    ids = ids_ref[...]
    weights = [jnp.sum(jnp.where(ids == ring(-d), shares, 0.0), axis=1, keepdims=True) for d in range(n)]
    for c, (start, size) in enumerate(cuts):
        mixed = weights[0] * zsend[c, z].astype(jnp.float32)
        for d in range(1, n):
            z_copies[c][d - 1].wait_recv()
            mixed += weights[d] * zrecv[c, d].astype(jnp.float32)
        out_ref[:, start:start + size] = mixed.astype(out_ref.dtype)
    for copy in started:
        copy.wait_send()


def fused_local(tokens, expert_ids, route_levels, gate_proj, up_proj, down_proj):
    rows, width = tokens.shape
    n = lax.axis_size("expert") // 2
    units = gate_proj.shape[2]
    pieces = 7
    cuts = column_cuts(width, pieces)
    nc, span, part = len(cuts), cuts[0][1], n * rows
    bf, f32 = jnp.bfloat16, jnp.float32
    vmem = pl.BlockSpec(memory_space=pltpu.VMEM)
    hbm = pl.BlockSpec(memory_space=pl.ANY)
    messages = 160
    return pl.pallas_call(
        functools.partial(fused, n, width * 4 // 7 // 128 * 128, cuts),
        out_shape=jax.ShapeDtypeStruct((rows, width), bf),
        in_specs=[vmem, vmem, vmem, hbm, hbm, hbm],
        out_specs=vmem,
        scratch_shapes=[
            pltpu.VMEM((2 * n, 2, rows, width), bf),
            pltpu.VMEM((width, units), bf),
            pltpu.VMEM((width, units), bf),
            pltpu.VMEM((units, width), bf),
            pltpu.VMEM((n, 2, 2, rows, units), f32),
            pltpu.VMEM((nc, 2 * part, span), f32),
            pltpu.VMEM((nc, 2 * part, span), bf),
            pltpu.VMEM((nc, 2 * part, span), bf),
            pltpu.VMEM((nc, part, span), bf),
            pltpu.VMEM((nc, part, span), bf),
            pltpu.VMEM((nc, n, rows, span), bf),
            pltpu.VMEM((nc, n, rows, span), bf),
            pltpu.SemaphoreType.DMA((messages,)),
            pltpu.SemaphoreType.DMA((messages,)),
            pltpu.SemaphoreType.DMA((3,)),
        ],
        compiler_params=pltpu.CompilerParams(collective_id=0, has_side_effects=True, vmem_limit_bytes=VMEM_BUDGET),
    )(expert_ids, route_levels, tokens, gate_proj, up_proj, down_proj)


def whole(tokens, expert_ids, route_levels, gate_proj, up_proj, down_proj):
    rows, width = tokens.shape
    groups = lax.axis_size("expert") // 2
    held = groups * rows * width * 64 + 6 * width * gate_proj.shape[2]
    if groups % 2 == 0 and lax.axis_size("sub") == 2 and width % (7 * 128) == 0 and held < VMEM_BUDGET:
        return fused_local(tokens, expert_ids, route_levels, gate_proj, up_proj, down_proj)
    return local(tokens, expert_ids, route_levels, gate_proj, up_proj, down_proj)


def solution(mesh):
    return jax.shard_map(
        whole,
        mesh=mesh,
        in_specs=(
            P(("replica", "expert", "sub"), None),
            P(("replica", "expert", "sub"), None),
            P(("replica", "expert", "sub"), None),
            P("expert", None, "sub"),
            P("expert", None, "sub"),
            P("expert", "sub", None),
        ),
        out_specs=P(("replica", "expert", "sub"), None),
        check_vma=False,
    )
```

```python
import functools
import jax
import jax.numpy as jnp
from jax import lax
from jax.experimental import pallas as pl
from jax.experimental.pallas import tpu as pltpu
from jax.sharding import PartitionSpec as P


def local(tokens, expert_ids, route_levels, gate_proj, up_proj, down_proj):
    rows_here, width = tokens.shape
    picks = expert_ids.shape[1]
    experts = lax.axis_size("expert") * lax.axis_size("sub") // 4
    capacity = rows_here * picks * 3 // (experts * 2)
    pair_count = rows_here * picks
    flat_ids = expert_ids.reshape(pair_count)
    onehot = (flat_ids[:, None] == jnp.arange(experts, dtype=jnp.int32)[None, :]).astype(jnp.int32)
    before = jnp.cumsum(onehot, axis=0, dtype=jnp.int32) - onehot
    slot_of = jnp.sum(before * onehot, axis=1)
    position = flat_ids * capacity + slot_of
    placed = (position[:, None] == jnp.arange(experts * capacity, dtype=jnp.int32)[None, :]).astype(
        jnp.float32
    )
    shares = route_levels.astype(jnp.float32)
    shares = shares / jnp.sum(shares, axis=1, keepdims=True)
    owner_rows = (
        jnp.arange(pair_count, dtype=jnp.int32)[None, :] // picks
        == jnp.arange(rows_here, dtype=jnp.int32)[:, None]
    ).astype(jnp.float32)
    sender = jnp.dot(owner_rows, placed, precision=lax.Precision.HIGHEST)
    weighting = jnp.dot(
        owner_rows * shares.reshape(1, pair_count), placed, precision=lax.Precision.HIGHEST
    )
    outgoing = jnp.dot(sender.T.astype(jnp.bfloat16), tokens, preferred_element_type=jnp.float32)
    outgoing = outgoing.astype(jnp.bfloat16).reshape(experts, 1, capacity, width)
    gate_local = gate_proj[0]
    up_local = up_proj[0]
    down_local = down_proj[0]
    buffer = jnp.broadcast_to(outgoing, (experts, 4, capacity, width)).reshape(
        4 * experts, capacity, width
    )
    arrived = lax.all_to_all(buffer, ("expert", "sub"), split_axis=0, concat_axis=0, tiled=True)
    items = arrived.shape[1]
    leading = arrived.shape[:-1]
    flat_rows = arrived.reshape(-1, width)
    gate_vals = jnp.dot(flat_rows, gate_local, preferred_element_type=jnp.float32)
    up_vals = jnp.dot(flat_rows, up_local, preferred_element_type=jnp.float32)
    hidden = (jax.nn.silu(gate_vals) * up_vals).astype(jnp.bfloat16)
    terms = jnp.dot(hidden, down_local, preferred_element_type=jnp.float32).astype(jnp.bfloat16)
    terms = terms.reshape(leading + (width,)).reshape(-1, 2, items, width)
    groups, _, items, _ = terms.shape
    flat_terms = terms.reshape(2 * groups, items, width)
    returned = lax.all_to_all(
        flat_terms, ("expert", "sub"), split_axis=0, concat_axis=0, tiled=True
    )
    results = jnp.sum(returned.reshape(experts, -1, capacity, width), axis=1, dtype=jnp.float32)
    rounded = lax.optimization_barrier(
        results.reshape(experts * capacity, width).astype(jnp.bfloat16)
    )
    mixed = jnp.dot(
        weighting,
        rounded.astype(jnp.float32),
        precision=lax.Precision.HIGHEST,
        preferred_element_type=jnp.float32,
    )
    return mixed.astype(jnp.bfloat16)


MESH = pl.DeviceIdType.MESH
VMEM_BUDGET = 60 * 1024 * 1024


def column_cuts(width, pieces):
    lanes = width // 128
    edges = [128 * (lanes * i // pieces) for i in range(pieces + 1)]
    return [(a, b - a) for a, b in zip(edges[:-1], edges[1:]) if b > a]


def column_cuts_from(start, width, pieces):
    return [(start + a, size) for a, size in column_cuts(width - start, pieces)]


def fused(groups, first_cols, rest_cols, cuts, ids_hbm, levels_hbm, tok_hbm, gate_hbm, up_hbm, down_hbm, out_ref,
          ids_ref, levels_ref, tok, gate_v, up_v, down_v, hid, keep, dsend, drecv, ysend, yrecv, zsend, zrecv,
          send_sem, recv_sem, local_sem):
    rows, width = tok_hbm.shape
    spot = lax.axis_index("expert")
    s = lax.axis_index("sub")
    z, h = spot // 2, spot % 2
    n = groups

    first_load = pltpu.make_async_copy(tok_hbm, tok.at[spot, s], local_sem.at[0])
    first_load.start()
    loads = [pltpu.make_async_copy(src, dst, local_sem.at[i + 1]) for i, (src, dst) in enumerate(
        ((ids_hbm, ids_ref), (levels_hbm, levels_ref),
         (gate_hbm.at[0], gate_v), (up_hbm.at[0], up_v), (down_hbm.at[0], down_v)))]

    def ring(step):
        return lax.rem(z + step + n, n)

    def at(group, half, core):
        return {"expert": group * 2 + half, "sub": core}

    sub_peer, half_peer = at(z, h, 1 - s), at(z, 1 - h, s)
    above, below = z + 1 < n, z > 0
    barrier = pltpu.get_barrier_semaphore()

    def greet(peer):
        pl.semaphore_signal(barrier, inc=1, device_id=peer, device_id_type=MESH)

    pl.when(above)(lambda: greet(at(z + 1, h, s)))
    pl.when(below)(lambda: greet(at(z - 1, h, s)))
    greet(half_peer)
    greet(sub_peer)
    for load in loads:
        load.start()
    first_load.wait()
    pl.semaphore_wait(barrier, 2 + above.astype(jnp.int32) + below.astype(jnp.int32))

    count = [0]
    endings = []

    def copy_of(i, src, dst, peer):
        return pltpu.make_async_remote_copy(src_ref=src, dst_ref=dst, send_sem=send_sem.at[i],
                                            recv_sem=recv_sem.at[i], device_id=peer, device_id_type=MESH)

    def send(src, dst, peer):
        i = count[0]
        count[0] += 1
        copy = copy_of(i, src, dst, peer)
        copy.start()
        endings.append(copy.wait_send)
        return copy

    def block(group, half, cols):
        return tok.at[group * 2 + half, s, :, pl.ds(cols[0], cols[1])]

    def when_send(group, half, cols, peer, cond):
        i = count[0]
        count[0] += 1
        part_of = block(group, half, cols)
        copy = copy_of(i, part_of, part_of, peer)

        def do(action):
            if cond is None:
                action()
            else:
                pl.when(cond)(action)
        do(copy.start)
        endings.append(lambda: do(copy.wait_send))
        return i

    def when_arrived(i, group, half, cols, cond):
        part_of = block(group, half, cols)
        copy = copy_of(i, part_of, part_of, sub_peer)
        if cond is None:
            copy.wait_recv()
        else:
            pl.when(cond)(copy.wait_recv)

    def climb(d, half, cols):
        return (when_send(z - d + 1, half, cols, at(z + 1, h, s), above & (z - d + 1 >= 0)),
                when_send(z + d - 1, half, cols, at(z - 1, h, s), below & (z + d - 1 < n)))

    crossing, turning = [], []

    def across(group, half, cols, cond=None):
        crossing.append((when_send(group, half, cols, sub_peer, cond), group, half, cols, cond))

    def turn(group, cols, cond=None):
        turning.append((when_send(group, h, cols, half_peer, cond), group, 1 - h, cols, cond))

    def turned(amount):
        for _ in range(amount):
            item = turning.pop(0)
            when_arrived(*item)
            across(*item[1:])

    first_turn = [when_send(z, h, cols, half_peer, None) for cols in first_cols]
    lines = [(h, cols) for cols in first_cols + rest_cols]
    steps = [climb(1, half, cols) for half, cols in lines]
    for cols in rest_cols:
        turn(z, cols)
    across(z, h, (0, width))
    for i, cols in zip(first_turn, first_cols):
        when_arrived(i, z, 1 - h, cols, None)
        lines.append((1 - h, cols))
        steps.append(climb(1, 1 - h, cols))
        across(z, 1 - h, cols)
    for d in range(1, n):
        later = []
        waiting = len(turning)
        for (half, cols), (rising, falling) in zip(lines, steps):
            low, high = z - d >= 0, z + d < n
            when_arrived(rising, z - d, half, cols, low)
            when_arrived(falling, z + d, half, cols, high)
            if d + 1 < n:
                later.append(climb(d + 1, half, cols))
            if cols in rest_cols:
                turn(z - d, cols, low)
                turn(z + d, cols, high)
            across(z - d, half, cols, low)
            across(z + d, half, cols, high)
        steps = later
        turned(waiting)
    turned(len(turning))
    for item in crossing:
        when_arrived(*item)
    for load in loads:
        load.wait()

    total = 4 * n * rows
    gate = jnp.zeros((total, gate_v.shape[1]), jnp.float32)
    up = jnp.zeros((total, up_v.shape[1]), jnp.float32)
    for start, size in cuts:
        lhs = tok[:, :, :, start:start + size].reshape(total, size)
        gate += jnp.dot(lhs, gate_v[start:start + size, :], preferred_element_type=jnp.float32)
        up += jnp.dot(lhs, up_v[start:start + size, :], preferred_element_type=jnp.float32)
    hid[...] = (jax.nn.silu(gate) * up).reshape(hid.shape)
    units = hid.shape[-1]
    ordered = jnp.concatenate([hid[:, half, core].reshape(n * rows, units)
                               for core in (1 - s, s) for half in (1 - h, h)], axis=0).astype(jnp.bfloat16)

    part, span = n * rows, max(size for _, size in cuts)
    d_copies, y_copies, z_copies = [], [], []
    for c, (start, size) in enumerate(cuts):
        terms = jnp.dot(ordered, down_v[:, start:start + size], preferred_element_type=jnp.float32)
        dsend[c] = terms[:2 * part].astype(jnp.bfloat16)
        keep[c] = terms[2 * part:]
        d_copies.append(send(dsend.at[c], drecv.at[c], sub_peer))
    for c in range(len(cuts)):
        d_copies[c].wait_recv()
        ysend[c] = (keep[c, :part] + drecv[c, :part].astype(jnp.float32)).astype(jnp.bfloat16)
        y_copies.append(send(ysend.at[c], yrecv.at[c], half_peer))
    for c in range(len(cuts)):
        y_copies[c].wait_recv()
        sums = (keep[c, part:] + drecv[c, part:].astype(jnp.float32)) + yrecv[c].astype(jnp.float32)
        zsend[c] = sums.reshape(n, rows, span).astype(jnp.bfloat16)
        z_copies.append([send(zsend.at[c, ring(d)], zrecv.at[c, d], at(ring(d), h, s)) for d in range(1, n)])
    levels = levels_ref[...].astype(jnp.float32)
    shares = levels / jnp.sum(levels, axis=0, keepdims=True)
    ids = ids_ref[...]
    eye = (lax.broadcasted_iota(jnp.int32, (rows, rows), 0) == lax.broadcasted_iota(jnp.int32, (rows, rows), 1))
    weights = []
    for d in range(n):
        flat = jnp.sum(jnp.where(ids == ring(-d), shares, 0.0), axis=0, keepdims=True)
        weights.append(jnp.sum(jnp.where(eye, flat, 0.0), axis=1, keepdims=True))
    for c, (start, size) in enumerate(cuts):
        mixed = weights[0] * zsend[c, z].astype(jnp.float32)
        for d in range(1, n):
            z_copies[c][d - 1].wait_recv()
            mixed += weights[d] * zrecv[c, d].astype(jnp.float32)
        out_ref[:, start:start + size] = mixed.astype(out_ref.dtype)
    for ending in endings:
        ending()


def fused_local(tokens, expert_ids, route_levels, gate_proj, up_proj, down_proj):
    rows, width = tokens.shape
    n = lax.axis_size("expert") // 2
    units = gate_proj.shape[2]
    pieces = 7
    cuts = column_cuts(width, pieces)
    nc, span, part = len(cuts), cuts[0][1], n * rows
    bf, f32 = jnp.bfloat16, jnp.float32
    vmem = pl.BlockSpec(memory_space=pltpu.VMEM)
    hbm = pl.BlockSpec(memory_space=pl.ANY)
    messages = 240
    return pl.pallas_call(
        functools.partial(fused, n, [cuts[0]], column_cuts_from(cuts[0][1], width, 3), cuts),
        out_shape=jax.ShapeDtypeStruct((rows, width), bf),
        in_specs=[hbm] * 6,
        out_specs=vmem,
        scratch_shapes=[
            pltpu.VMEM(expert_ids.shape[::-1], jnp.int32),
            pltpu.VMEM(expert_ids.shape[::-1], jnp.int32),
            pltpu.VMEM((2 * n, 2, rows, width), bf),
            pltpu.VMEM((width, units), bf),
            pltpu.VMEM((width, units), bf),
            pltpu.VMEM((units, width), bf),
            pltpu.VMEM((n, 2, 2, rows, units), f32),
            pltpu.VMEM((nc, 2 * part, span), f32),
            pltpu.VMEM((nc, 2 * part, span), bf),
            pltpu.VMEM((nc, 2 * part, span), bf),
            pltpu.VMEM((nc, part, span), bf),
            pltpu.VMEM((nc, part, span), bf),
            pltpu.VMEM((nc, n, rows, span), bf),
            pltpu.VMEM((nc, n, rows, span), bf),
            pltpu.SemaphoreType.DMA((messages,)),
            pltpu.SemaphoreType.DMA((messages,)),
            pltpu.SemaphoreType.DMA((6,)),
        ],
        compiler_params=pltpu.CompilerParams(collective_id=0, has_side_effects=True, vmem_limit_bytes=VMEM_BUDGET),
    )(expert_ids.T, route_levels.T, tokens, gate_proj, up_proj, down_proj)


def whole(tokens, expert_ids, route_levels, gate_proj, up_proj, down_proj):
    rows, width = tokens.shape
    groups = lax.axis_size("expert") // 2
    held = groups * rows * width * 64 + 6 * width * gate_proj.shape[2]
    if groups % 2 == 0 and lax.axis_size("sub") == 2 and width % (7 * 128) == 0 and held < VMEM_BUDGET:
        return fused_local(tokens, expert_ids, route_levels, gate_proj, up_proj, down_proj)
    return local(tokens, expert_ids, route_levels, gate_proj, up_proj, down_proj)


def solution(mesh):
    return jax.shard_map(
        whole,
        mesh=mesh,
        in_specs=(
            P(("replica", "expert", "sub"), None),
            P(("replica", "expert", "sub"), None),
            P(("replica", "expert", "sub"), None),
            P("expert", None, "sub"),
            P("expert", None, "sub"),
            P("expert", "sub", None),
        ),
        out_specs=P(("replica", "expert", "sub"), None),
        check_vma=False,
    )
```

```python
import functools
import jax
import jax.numpy as jnp
from jax import lax
from jax.experimental import pallas as pl
from jax.experimental.pallas import tpu as pltpu
from jax.sharding import PartitionSpec as P


def local(tokens, expert_ids, route_levels, gate_proj, up_proj, down_proj):
    rows_here, width = tokens.shape
    picks = expert_ids.shape[1]
    experts = lax.axis_size("expert") * lax.axis_size("sub") // 4
    capacity = rows_here * picks * 3 // (experts * 2)
    pair_count = rows_here * picks
    flat_ids = expert_ids.reshape(pair_count)
    onehot = (flat_ids[:, None] == jnp.arange(experts, dtype=jnp.int32)[None, :]).astype(jnp.int32)
    before = jnp.cumsum(onehot, axis=0, dtype=jnp.int32) - onehot
    slot_of = jnp.sum(before * onehot, axis=1)
    position = flat_ids * capacity + slot_of
    placed = (position[:, None] == jnp.arange(experts * capacity, dtype=jnp.int32)[None, :]).astype(
        jnp.float32
    )
    shares = route_levels.astype(jnp.float32)
    shares = shares / jnp.sum(shares, axis=1, keepdims=True)
    owner_rows = (
        jnp.arange(pair_count, dtype=jnp.int32)[None, :] // picks
        == jnp.arange(rows_here, dtype=jnp.int32)[:, None]
    ).astype(jnp.float32)
    sender = jnp.dot(owner_rows, placed, precision=lax.Precision.HIGHEST)
    weighting = jnp.dot(
        owner_rows * shares.reshape(1, pair_count), placed, precision=lax.Precision.HIGHEST
    )
    outgoing = jnp.dot(sender.T.astype(jnp.bfloat16), tokens, preferred_element_type=jnp.float32)
    outgoing = outgoing.astype(jnp.bfloat16).reshape(experts, 1, capacity, width)
    gate_local = gate_proj[0]
    up_local = up_proj[0]
    down_local = down_proj[0]
    buffer = jnp.broadcast_to(outgoing, (experts, 4, capacity, width)).reshape(
        4 * experts, capacity, width
    )
    arrived = lax.all_to_all(buffer, ("expert", "sub"), split_axis=0, concat_axis=0, tiled=True)
    items = arrived.shape[1]
    leading = arrived.shape[:-1]
    flat_rows = arrived.reshape(-1, width)
    gate_vals = jnp.dot(flat_rows, gate_local, preferred_element_type=jnp.float32)
    up_vals = jnp.dot(flat_rows, up_local, preferred_element_type=jnp.float32)
    hidden = (jax.nn.silu(gate_vals) * up_vals).astype(jnp.bfloat16)
    terms = jnp.dot(hidden, down_local, preferred_element_type=jnp.float32).astype(jnp.bfloat16)
    terms = terms.reshape(leading + (width,)).reshape(-1, 2, items, width)
    groups, _, items, _ = terms.shape
    flat_terms = terms.reshape(2 * groups, items, width)
    returned = lax.all_to_all(
        flat_terms, ("expert", "sub"), split_axis=0, concat_axis=0, tiled=True
    )
    results = jnp.sum(returned.reshape(experts, -1, capacity, width), axis=1, dtype=jnp.float32)
    rounded = lax.optimization_barrier(
        results.reshape(experts * capacity, width).astype(jnp.bfloat16)
    )
    mixed = jnp.dot(
        weighting,
        rounded.astype(jnp.float32),
        precision=lax.Precision.HIGHEST,
        preferred_element_type=jnp.float32,
    )
    return mixed.astype(jnp.bfloat16)


MESH = pl.DeviceIdType.MESH
VMEM_BUDGET = 60 * 1024 * 1024


def column_cuts(width, pieces):
    lanes = width // 128
    edges = [128 * (lanes * i // pieces) for i in range(pieces + 1)]
    return [(a, b - a) for a, b in zip(edges[:-1], edges[1:]) if b > a]


def column_cuts_from(start, width, pieces):
    return [(start + a, size) for a, size in column_cuts(width - start, pieces)]


def shrinking_cuts(width):
    shares, lanes, edges = (3, 6, 6, 6, 4, 3), width // 128, [0]
    for share in shares:
        edges.append(edges[-1] + share)
    edges = [128 * (lanes * edge // edges[-1]) for edge in edges]
    return [(a, b - a) for a, b in zip(edges[:-1], edges[1:])]


def fused(groups, rest_cols, cuts, tails, ids_hbm, levels_hbm, tok_hbm, gate_hbm, up_hbm, down_hbm, out_ref,
          ids_ref, levels_ref, tok, gate_v, up_v, down_v, hid, keep, dsend, drecv, ysend, yrecv, zsend, zrecv,
          send_sem, recv_sem, local_sem):
    rows, width = tok_hbm.shape
    spot = lax.axis_index("expert")
    s = lax.axis_index("sub")
    z, h = spot // 2, spot % 2
    n = groups

    first_load = pltpu.make_async_copy(tok_hbm, tok.at[spot, s], local_sem.at[0])
    first_load.start()
    loads = [pltpu.make_async_copy(src, dst, local_sem.at[i + 1]) for i, (src, dst) in enumerate(
        ((ids_hbm, ids_ref), (levels_hbm, levels_ref),
         (gate_hbm.at[0], gate_v), (up_hbm.at[0], up_v), (down_hbm.at[0], down_v)))]

    def ring(step):
        return lax.rem(z + step + n, n)

    def at(group, half, core):
        return {"expert": group * 2 + half, "sub": core}

    sub_peer, half_peer = at(z, h, 1 - s), at(z, 1 - h, s)
    above, below = z + 1 < n, z > 0
    barrier = pltpu.get_barrier_semaphore()

    def greet(peer):
        pl.semaphore_signal(barrier, inc=1, device_id=peer, device_id_type=MESH)

    pl.when(above)(lambda: greet(at(z + 1, h, s)))
    pl.when(below)(lambda: greet(at(z - 1, h, s)))
    greet(half_peer)
    greet(sub_peer)
    for load in loads:
        load.start()
    first_load.wait()
    pl.semaphore_wait(barrier, 2 + above.astype(jnp.int32) + below.astype(jnp.int32))

    count = [0]
    endings = []

    def slots(amount):
        count[0] += amount
        return count[0] - amount

    def copy_of(i, j, src, dst, peer):
        return pltpu.make_async_remote_copy(src_ref=src, dst_ref=dst, send_sem=send_sem.at[i],
                                            recv_sem=recv_sem.at[j], device_id=peer, device_id_type=MESH)

    def send(src, dst, peer):
        i = slots(1)
        copy = copy_of(i, i, src, dst, peer)
        copy.start()
        endings.append(copy.wait_send)
        return copy

    def block(group, half, cols):
        return tok.at[group * 2 + half, s, :, pl.ds(cols[0], cols[1])]

    def do(cond, action):
        if cond is None:
            action()
        else:
            pl.when(cond)(action)

    def when_send(i, j, group, half, cols, peer, cond=None):
        part_of = block(group, half, cols)
        copy = copy_of(i, j, part_of, part_of, peer)
        do(cond, copy.start)
        endings.append(lambda: do(cond, copy.wait_send))

    def when_arrived(j, group, half, cols, cond=None):
        part_of = block(group, half, cols)
        do(cond, copy_of(j, j, part_of, part_of, sub_peer).wait_recv)

    def climb(d, base, half, cols):
        low, high = z - d + 1, z + d - 1
        when_send(base + low, base + low, low, half, cols, at(z + 1, h, s), above & (low >= 0))
        when_send(base + (n if d == 1 else high), base + high, high, half, cols, at(z - 1, h, s), below & (high < n))

    crossing, turning = [], []
    front = (0, rest_cols[0][0])
    back = (front[1], width - front[1])
    near_base, far_base, back_base = slots(n), slots(n), slots(n)
    turn_base = [slots(n) for _ in rest_cols]

    def across(base, group, half, cols, cond=None):
        when_send(base + group, base + group, group, half, cols, sub_peer, cond)
        crossing.append((base + group, group, half, cols, cond))

    def turn(k, group, cols, cond=None):
        when_send(turn_base[k] + group, turn_base[k] + group, group, h, cols, half_peer, cond)
        turning.append((turn_base[k] + group, group, 1 - h, cols, cond))

    def turned(amount):
        for _ in range(amount):
            item = turning.pop(0)
            when_arrived(*item)
            if item[3] == rest_cols[-1]:
                across(back_base, item[1], 1 - h, back, item[4])

    first_base = slots(1)
    when_send(first_base, first_base, z, h, front, half_peer)
    lines = [(slots(n + 1), h, cols) for cols in rest_cols + [front]]
    for line in lines:
        climb(1, *line)
    for k, cols in enumerate(rest_cols):
        turn(k, z, cols)
    across(near_base, z, h, (0, width))
    when_arrived(first_base, z, 1 - h, front)
    lines.append((slots(n + 1), 1 - h, front))
    climb(1, *lines[-1])
    across(far_base, z, 1 - h, front)
    for d in range(1, n):
        waiting = len(turning)
        low, high = z - d >= 0, z + d < n
        for base, half, cols in lines:
            when_arrived(base + z - d, z - d, half, cols, low)
            when_arrived(base + z + d, z + d, half, cols, high)
            if d + 1 < n:
                climb(d + 1, base, half, cols)
            if cols in rest_cols:
                k = rest_cols.index(cols)
                turn(k, z - d, cols, low)
                turn(k, z + d, cols, high)
            elif half is h:
                across(near_base, z - d, h, (0, width), low)
                across(near_base, z + d, h, (0, width), high)
            else:
                across(far_base, z - d, half, cols, low)
                across(far_base, z + d, half, cols, high)
        turned(waiting)
    turned(len(turning))
    for item in crossing:
        when_arrived(*item)
    for load in loads:
        load.wait()

    total = 4 * n * rows
    gate = jnp.zeros((total, gate_v.shape[1]), jnp.float32)
    up = jnp.zeros((total, up_v.shape[1]), jnp.float32)
    for start, size in cuts:
        lhs = tok[:, :, :, start:start + size].reshape(total, size)
        gate += jnp.dot(lhs, gate_v[start:start + size, :], preferred_element_type=jnp.float32)
        up += jnp.dot(lhs, up_v[start:start + size, :], preferred_element_type=jnp.float32)
    hid[...] = (jax.nn.silu(gate) * up).reshape(hid.shape)
    units = hid.shape[-1]
    ordered = jnp.concatenate([hid[:, half, core].reshape(n * rows, units)
                               for core in (1 - s, s) for half in (1 - h, h)], axis=0).astype(jnp.bfloat16)

    part = n * rows
    d_copies, y_copies, z_copies = [], [], []

    def project(c):
        start, size = tails[c]
        cols = pl.ds(start, size)
        terms = jnp.dot(ordered, down_v[:, start:start + size], preferred_element_type=jnp.float32)
        dsend[:, cols] = terms[:2 * part].astype(jnp.bfloat16)
        keep[:, cols] = terms[2 * part:]
        d_copies.append(send(dsend.at[:, cols], drecv.at[:, cols], sub_peer))

    def join_cores(c):
        cols = pl.ds(*tails[c])
        d_copies[c].wait_recv()
        ysend[:, cols] = (keep[:part, cols] + drecv[:part, cols].astype(jnp.float32)).astype(jnp.bfloat16)
        y_copies.append(send(ysend.at[:, cols], yrecv.at[:, cols], half_peer))

    def join_halves(c):
        cols = pl.ds(*tails[c])
        y_copies[c].wait_recv()
        sums = keep[part:, cols] + drecv[part:, cols].astype(jnp.float32) + yrecv[:, cols].astype(jnp.float32)
        zsend[:, :, cols] = sums.reshape(n, rows, tails[c][1]).astype(jnp.bfloat16)
        z_copies.append([send(zsend.at[ring(d), :, cols], zrecv.at[d, :, cols], at(ring(d), h, s))
                         for d in range(1, n)])

    for c in range(len(tails) + 2):
        if c < len(tails):
            project(c)
        if c >= 2:
            join_cores(c - 2)
    for c in range(len(tails)):
        join_halves(c)
    levels = levels_ref[...].astype(jnp.float32)
    shares = levels / jnp.sum(levels, axis=0, keepdims=True)
    ids = ids_ref[...]
    eye = (lax.broadcasted_iota(jnp.int32, (rows, rows), 0) == lax.broadcasted_iota(jnp.int32, (rows, rows), 1))
    weights = []
    for d in range(n):
        flat = jnp.sum(jnp.where(ids == ring(-d), shares, 0.0), axis=0, keepdims=True)
        weights.append(jnp.sum(jnp.where(eye, flat, 0.0), axis=1, keepdims=True))
    for c, (start, size) in enumerate(tails):
        cols = pl.ds(start, size)
        mixed = weights[0] * zsend[z, :, cols].astype(jnp.float32)
        for d in range(1, n):
            z_copies[c][d - 1].wait_recv()
            mixed += weights[d] * zrecv[d, :, cols].astype(jnp.float32)
        out_ref[:, cols] = mixed.astype(out_ref.dtype)
    for ending in endings:
        ending()


def fused_local(tokens, expert_ids, route_levels, gate_proj, up_proj, down_proj):
    rows, width = tokens.shape
    n = lax.axis_size("expert") // 2
    units = gate_proj.shape[2]
    pieces = 7
    cuts = column_cuts(width, pieces)
    span, part = cuts[0][1], n * rows
    tails = shrinking_cuts(width)
    nc = len(tails)
    bf, f32 = jnp.bfloat16, jnp.float32
    vmem = pl.BlockSpec(memory_space=pltpu.VMEM)
    hbm = pl.BlockSpec(memory_space=pl.ANY)
    rest = column_cuts_from(span, width, 3)
    messages = (3 + len(rest)) * n + (len(rest) + 2) * (n + 1) + 1 + nc * (n + 1)
    return pl.pallas_call(
        functools.partial(fused, n, rest, cuts, tails),
        out_shape=jax.ShapeDtypeStruct((rows, width), bf),
        in_specs=[hbm] * 6,
        out_specs=vmem,
        scratch_shapes=[
            pltpu.VMEM(expert_ids.shape[::-1], jnp.int32),
            pltpu.VMEM(expert_ids.shape[::-1], jnp.int32),
            pltpu.VMEM((2 * n, 2, rows, width), bf),
            pltpu.VMEM((width, units), bf),
            pltpu.VMEM((width, units), bf),
            pltpu.VMEM((units, width), bf),
            pltpu.VMEM((n, 2, 2, rows, units), f32),
            pltpu.VMEM((2 * part, width), f32),
            pltpu.VMEM((2 * part, width), bf),
            pltpu.VMEM((2 * part, width), bf),
            pltpu.VMEM((part, width), bf),
            pltpu.VMEM((part, width), bf),
            pltpu.VMEM((n, rows, width), bf),
            pltpu.VMEM((n, rows, width), bf),
            pltpu.SemaphoreType.DMA((messages,)),
            pltpu.SemaphoreType.DMA((messages,)),
            pltpu.SemaphoreType.DMA((6,)),
        ],
        compiler_params=pltpu.CompilerParams(collective_id=0, has_side_effects=True, vmem_limit_bytes=VMEM_BUDGET),
    )(expert_ids.T, route_levels.T, tokens, gate_proj, up_proj, down_proj)


def whole(tokens, expert_ids, route_levels, gate_proj, up_proj, down_proj):
    rows, width = tokens.shape
    groups = lax.axis_size("expert") // 2
    held = groups * rows * width * 64 + 6 * width * gate_proj.shape[2]
    if groups % 2 == 0 and lax.axis_size("sub") == 2 and width % (7 * 128) == 0 and held < VMEM_BUDGET:
        return fused_local(tokens, expert_ids, route_levels, gate_proj, up_proj, down_proj)
    return local(tokens, expert_ids, route_levels, gate_proj, up_proj, down_proj)


def solution(mesh):
    return jax.shard_map(
        whole,
        mesh=mesh,
        in_specs=(
            P(("replica", "expert", "sub"), None),
            P(("replica", "expert", "sub"), None),
            P(("replica", "expert", "sub"), None),
            P("expert", None, "sub"),
            P("expert", None, "sub"),
            P("expert", "sub", None),
        ),
        out_specs=P(("replica", "expert", "sub"), None),
        check_vma=False,
    )
```
